32 devices in a mesh: elem: 8 (over z, y), bucket: 4 (over x, core).
Axes of the slice: x: 2, y: 2, z: 4, core: 2. Of those that a mesh axis runs over, the one named last changes fastest.
Arguments:
- node_data: float32 [24, 98304], P(None, 'elem'), may hold values from -6 to 6
- eroded: int32 [4096], P('elem'), may hold values from 0 to 2047, as said below
- bucket_map: int32 [98304], P('elem'), may hold values from 0 to 63, as said below
- seg_point: float32 [64, 3, 512], P('elem', None, 'bucket'), may hold values from -3 to 3
- seg_angle: float32 [64, 2, 512], P('elem', None, 'bucket'), may hold values from -3.140625 to 3.140625
Outputs:
- face_force: float32 [3, 24576], P(None, 'elem')
The draws below stay inside these ranges and needn't reach their ends.
Inputs may be any that keep to these rules, and one draw needn't show every extreme that they name: `eroded`: the 512 entries of one index of elem are distinct local element numbers. `bucket_map`: among the faces of the elements listed in eroded, those of one index of elem name one bucket at most 80 times; in every draw some bucket is named exactly 80 times by every index of elem.
All inputs are finite; a program needn't handle non-finite values.
Results may differ from the reference program's by a relative error of at most 0.00012.
Values sent between devices are 32-bit elements; how exact they have to be, the bound alone decides.
A program may use at most 64 MiB of HBM per device.

```python
import jax
import jax.numpy as jnp
from jax import lax

ELEM_DEV = 2048
ERODE_DEV = 512
SLOT = 80
BUCKETS = 64
SEGS = 512
FACES = 98304
UNCOVERED = 24576
N_ELEM = 8


def erosion_plan(key):
    plan_key = jax.random.fold_in(key, 11)
    elem_key, pool_key, hot_key, fill_key = jax.random.split(plan_key, 4)
    elem_iota = jnp.arange(ELEM_DEV, dtype=jnp.int32)
    elem_scores = jax.random.randint(elem_key, (N_ELEM, ELEM_DEV), 0, 65536, dtype=jnp.int32) * ELEM_DEV + elem_iota[None, :]
    eroded = jnp.argsort(elem_scores, axis=1)[:, :ERODE_DEV].astype(jnp.int32)
    pool_size = BUCKETS * SLOT
    pool_iota = jnp.arange(pool_size, dtype=jnp.int32)
    pool_ids = pool_iota // SLOT
    hot_bucket = jax.random.randint(hot_key, (), 0, BUCKETS, dtype=jnp.int32)
    scores = jax.random.randint(pool_key, (N_ELEM, pool_size), 0, 65536, dtype=jnp.int32) * pool_size + pool_iota[None, :]
    scores = jnp.where((pool_ids == hot_bucket)[None, :], pool_iota[None, :] - pool_size, scores)
    pool_order = jnp.argsort(scores, axis=1)[:, :6 * ERODE_DEV]
    chosen = pool_ids[pool_order].astype(jnp.int32)
    background = jax.random.randint(fill_key, (N_ELEM, 6 * ELEM_DEV), 0, BUCKETS, dtype=jnp.int32)
    sides = jnp.arange(6, dtype=jnp.int32)
    face_index = (6 * eroded[:, :, None] + sides[None, None, :]).reshape(N_ELEM, 6 * ERODE_DEV)
    device_rows = jnp.broadcast_to(jnp.arange(N_ELEM, dtype=jnp.int32)[:, None], face_index.shape)
    bucket_map = background.at[device_rows, face_index].set(chosen)
    return (eroded.reshape(-1), bucket_map.reshape(-1))


def draw_eroded(key, part):
    return erosion_plan(key)[0]


def draw_bucket_map(key, part):
    return erosion_plan(key)[1]


def level_of(stream_key, dims, cuts, least, top_value):
    level = 1.0
    for axis_at, shards_of in cuts:
        heights = jax.random.uniform(jax.random.fold_in(jax.random.fold_in(stream_key, 6), axis_at), (shards_of,), jnp.float32, least / len(cuts), top_value / len(cuts))
        level = level * jnp.repeat(jnp.exp(heights), dims[axis_at] // shards_of).reshape((-1,) + (1,) * (len(dims) - 1 - axis_at))
    return level


def normal_values(own_key, shape, deviation, most, shards=(), held_as=jnp.bfloat16):
    factor_of = level_of(own_key, shape, shards, -0.22, 0.18) if shards else 1.0
    entries = jax.random.normal(own_key, shape, jnp.float32) * deviation * factor_of
    return jnp.minimum(jnp.maximum(entries, -most), most).astype(held_as)


def setup_inputs(seed: int = 0) -> dict:
    key_list = jax.random.split(jax.random.key(seed), 6)
    node_data = normal_values(key_list[0], (24, FACES), 1.0, 6.0, ((1, 8),), jnp.float32)
    eroded = draw_eroded(jax.random.fold_in(key_list[5], 71), 0)
    bucket_map = draw_bucket_map(jax.random.fold_in(key_list[5], 71), 0)
    seg_point = normal_values(key_list[3], (BUCKETS, 3, SEGS), 0.5, 3.0, ((0, 8), (2, 4)), jnp.float32)
    seg_angle = jnp.clip(jax.random.uniform(key_list[4], (BUCKETS, 2, SEGS), jnp.float32, -3.140625, 3.140625), -3.140625, 3.140625)
    return dict(node_data=node_data, eroded=eroded, bucket_map=bucket_map, seg_point=seg_point, seg_angle=seg_angle)


STIFFNESS = 20.0
DAMPING = 0.5

def face_geometry(payload):
    corner = payload[0:12].reshape(4, 3, -1)
    motion = payload[12:24].reshape(4, 3, -1)
    centroid = 0.25 * (corner[0] + corner[1] + corner[2] + corner[3])
    first_edge = corner[2] - corner[0]
    second_edge = corner[3] - corner[1]
    area_x = 0.5 * (first_edge[1] * second_edge[2] - first_edge[2] * second_edge[1])
    area_y = 0.5 * (first_edge[2] * second_edge[0] - first_edge[0] * second_edge[2])
    area_z = 0.5 * (first_edge[0] * second_edge[1] - first_edge[1] * second_edge[0])
    velocity = 0.25 * (motion[0] + motion[1] + motion[2] + motion[3])
    return jnp.concatenate([centroid, jnp.stack([area_x, area_y, area_z]), velocity], axis=0)

def unit_normal(angles):
    return jnp.stack([jnp.cos(angles[:, 0]) * jnp.sin(angles[:, 1]), jnp.sin(angles[:, 0]) * jnp.sin(angles[:, 1]), jnp.cos(angles[:, 1])], axis=1)

def penalty_terms(geometry, point, normal, stiff):
    offset = geometry[0:3, :, None] - point
    dist_sq = offset[0] * offset[0] + offset[1] * offset[1] + offset[2] * offset[2]
    gap_value = offset[0] * normal[0] + offset[1] * normal[1] + offset[2] * normal[2]
    closing = geometry[6][:, None] * normal[0] + geometry[7][:, None] * normal[1] + geometry[8][:, None] * normal[2]
    projected = jnp.abs(geometry[3][:, None] * normal[0] + geometry[4][:, None] * normal[1] + geometry[5][:, None] * normal[2])
    depth_in = jnp.maximum(-gap_value, 0.0)
    weight = jnp.exp(-0.5 * dist_sq)
    return weight * depth_in * (stiff - DAMPING * closing) * projected

def reference(node_data, eroded, bucket_map, seg_point, seg_angle):
    local = eroded.reshape(N_ELEM, ERODE_DEV)
    sides = jnp.arange(6, dtype=jnp.int32)
    face_local = (6 * local[:, :, None] + sides[None, None, :]).reshape(N_ELEM, 6 * ERODE_DEV)
    offsets = (jnp.arange(N_ELEM, dtype=jnp.int32) * (6 * ELEM_DEV)).astype(jnp.int32)
    face_global = (face_local + offsets[:, None]).reshape(-1).astype(jnp.int32)
    bucket = bucket_map[face_global]
    geometry = face_geometry(node_data[:, face_global])
    counts = jnp.zeros((BUCKETS,), jnp.float32).at[bucket].add(1.0)
    stiffness = STIFFNESS * lax.rsqrt(jnp.maximum(counts, 1.0))
    normal_all = unit_normal(seg_angle)
    block_count = UNCOVERED // 128
    geo_blocks = geometry.reshape(9, block_count, 128).transpose(1, 0, 2)
    id_blocks = bucket.reshape(block_count, 128)

    def block_force(items):
        geo, block_ids = items
        point = seg_point[block_ids].transpose(1, 0, 2)
        normal = normal_all[block_ids].transpose(1, 0, 2)
        stiff = stiffness[block_ids][:, None]
        traction = penalty_terms(geo, point, normal, stiff)
        return lax.optimization_barrier(jnp.sum(traction[None, :, :] * normal, axis=2))
    forces = lax.map(block_force, (geo_blocks, id_blocks))
    return forces.transpose(1, 0, 2).reshape(3, UNCOVERED)
```

```python
import functools

import jax
import jax.numpy as jnp
from jax import lax
from jax.experimental import pallas as pl
from jax.experimental.pallas import tpu as pltpu
from jax.sharding import PartitionSpec as P

STIFFNESS = 20.0
DAMPING = 0.5
LANES = 128
SIDES = 6
BLOCK = SIDES * LANES
ROWS = 32
F32 = jnp.float32
BF16 = jnp.bfloat16


def split3(x):
    hi = x.astype(BF16).astype(F32)
    rest = x - hi
    mid = rest.astype(BF16).astype(F32)
    return hi, mid, rest - mid


def sin_cos(x):
    k = jnp.floor(x * 0.6366197723675814 + 0.5)
    r = x - k * 1.5703125
    r = r - k * 4.837512969970703125e-4
    r = r - k * 7.54978995489188216e-8
    z = r * r
    s = ((-1.9515295891e-4 * z + 8.3321608736e-3) * z - 1.6666654611e-1) * z * r + r
    c = ((2.443315711809948e-5 * z - 1.388731625493765e-3) * z + 4.166664568298827e-2) * z * z
    c = c - 0.5 * z + 1.0
    q = k.astype(jnp.int32) & 3
    odd = (q & 1) == 1
    sin = jnp.where(odd, c, s)
    cos = jnp.where(odd, s, c)
    sin = jnp.where(q >= 2, -sin, sin)
    cos = jnp.where((q == 1) | (q == 2), -cos, cos)
    return sin, cos


def mm(a, b, contract=((1,), (0,))):
    return lax.dot_general(a, b, (contract, ((), ())), preferred_element_type=F32)


def kernel(
    n_elem, n_buck, node, eroded, bmap, spoint, sangle, out,
    perm, pick, rows, faces, geo, onehot, points, angles, seg_t, counts, sums_f, parts, inter,
    seg_send, seg_recv, cnt_send, cnt_recv, par_send, par_recv,
):
    me = lax.axis_index("elem")
    mb = lax.axis_index("bucket")
    own = spoint.shape[0]
    buckets = own * n_elem
    count = eroded.shape[1]
    jblocks = count // LANES
    blocks = node.shape[1] // BLOCK

    barrier = pltpu.get_barrier_semaphore()
    for d in range(1, n_elem):
        pl.semaphore_signal(
            barrier, inc=1, device_id={"elem": lax.rem(me + d, n_elem)},
            device_id_type=pl.DeviceIdType.MESH,
        )
    for d in range(1, n_buck):
        pl.semaphore_signal(
            barrier, inc=1, device_id={"bucket": lax.rem(mb + d, n_buck)},
            device_id_type=pl.DeviceIdType.MESH,
        )

    col = lax.broadcasted_iota(jnp.int32, (1, BLOCK), 1)
    source = SIDES * (col & (LANES - 1)) + (col // LANES)
    for i in range(BLOCK // 256):
        r = lax.broadcasted_iota(jnp.int32, (256, BLOCK), 0) + i * 256
        perm[i * 256:(i + 1) * 256, :] = jnp.where(r == source, 1.0, 0.0).astype(BF16)

    group = 4
    for g in range(blocks // group):
        stack = []
        for i in range(g * group, (g + 1) * group):
            lanes = slice(i * BLOCK, (i + 1) * BLOCK)
            ids = jnp.broadcast_to(bmap[:, lanes].astype(F32), (ROWS - 24, BLOCK))
            stack += [v.astype(BF16) for v in split3(jnp.concatenate([node[:, lanes], ids], axis=0))]
        apart = mm(jnp.concatenate(stack, axis=0), perm[...]).astype(BF16)
        for i in range(group):
            at = (g * group + i) * LANES
            for p in range(3):
                for s in range(SIDES):
                    top = (p * SIDES + s) * ROWS
                    r0 = (i * 3 + p) * ROWS
                    rows[top:top + ROWS, at:at + LANES] = apart[
                        r0:r0 + ROWS, s * LANES:(s + 1) * LANES
                    ]

    pl.semaphore_wait(barrier, n_elem + n_buck - 2)

    def seg_copies(slot, d, owner, target):
        at = pl.ds(owner * own, own)
        return [
            pltpu.make_async_remote_copy(
                src_ref=src, dst_ref=dst.at[at],
                send_sem=seg_send.at[i, slot], recv_sem=seg_recv.at[i, slot],
                device_id={"elem": target}, device_id_type=pl.DeviceIdType.MESH,
            )
            for i, (src, dst) in enumerate([(spoint, points), (sangle, angles)])
        ]

    for d in range(1, n_elem):
        for c in seg_copies(d - 1, d, me, lax.rem(me + d, n_elem)):
            c.start()
    points[pl.ds(me * own, own)] = spoint[...]
    angles[pl.ds(me * own, own)] = sangle[...]

    for i in range(pick.shape[0] // 256):
        r = lax.broadcasted_iota(jnp.int32, (256, count), 0) + i * 256
        pick[i * 256:(i + 1) * 256, :] = jnp.where(r == eroded[...], 1.0, 0.0).astype(BF16)
    taken = mm(rows[...], pick[...])
    third = SIDES * ROWS
    taken = (taken[0:third] + taken[third:2 * third]) + taken[2 * third:3 * third]
    for s in range(SIDES):
        faces[s] = taken[s * ROWS:(s + 1) * ROWS]

    ones = jnp.ones((8, count), BF16)
    chunk = min(buckets, LANES)
    for b in range(0, buckets, chunk):
        iota = lax.broadcasted_iota(jnp.int32, (chunk, count), 0) + b
        total = jnp.zeros((chunk, count), F32)
        for s in range(SIDES):
            ids = faces[s, 24:25, :].astype(jnp.int32)
            hot = jnp.where(iota == ids, 1.0, 0.0)
            total = total + hot
            onehot[b:b + chunk, s * count:(s + 1) * count] = hot.astype(BF16)
        if chunk < LANES:
            total = jnp.concatenate([total, jnp.zeros((LANES - chunk, count), F32)], axis=0)
        counts[me, :, b:b + LANES] = mm(ones, total.astype(BF16), ((1,), (1,)))

    def cnt_copy(slot, owner, target):
        return pltpu.make_async_remote_copy(
            src_ref=counts.at[owner], dst_ref=counts.at[owner],
            send_sem=cnt_send.at[slot], recv_sem=cnt_recv.at[slot],
            device_id={"elem": target}, device_id_type=pl.DeviceIdType.MESH,
        )

    for d in range(1, n_elem):
        cnt_copy(d - 1, me, lax.rem(me + d, n_elem)).start()

    c = [faces[:, i, :] for i in range(24)]
    e1 = [c[6 + i] - c[i] for i in range(3)]
    e2 = [c[9 + i] - c[3 + i] for i in range(3)]
    for i in range(3):
        j, k = (i + 1) % 3, (i + 2) % 3
        geo[:, i, :] = 0.25 * (c[i] + c[3 + i] + c[6 + i] + c[9 + i])
        geo[:, 3 + i, :] = 0.5 * (e1[j] * e2[k] - e1[k] * e2[j])
        geo[:, 6 + i, :] = 0.25 * (c[12 + i] + c[15 + i] + c[18 + i] + c[21 + i])

    for d in range(1, n_elem):
        for cp in seg_copies(d - 1, d, lax.rem(me + n_elem - d, n_elem), me):
            cp.wait_recv()
    chunk = min(buckets, LANES // 2)

    def lay_out(b):
        at = pl.ds(b * chunk, chunk)
        sin0, cos0 = sin_cos(angles[at, 0, :])
        sin1, cos1 = sin_cos(angles[at, 1, :])
        values = [points[at, i, :] for i in range(3)] + [cos0 * sin1, sin0 * sin1, cos1]
        for i, v in enumerate(values):
            stack = jnp.concatenate(list(split3(v)) + [jnp.zeros_like(v)], axis=0)
            lanes = pl.ds(pl.multiple_of(b * 4 * chunk, LANES), 4 * chunk)
            seg_t[i * LANES:(i + 1) * LANES, lanes] = stack.T.astype(BF16)

    if buckets == chunk:
        lay_out(0)
    else:
        pl.loop(0, buckets // chunk)(lay_out)

    half = 256
    halves = count // half

    def step(it, carry):
        s = it // halves
        h = it % halves
        hot = onehot[:, pl.ds(pl.multiple_of(it * half, half), half)]
        hot = [hot[b:b + chunk] for b in range(0, buckets, chunk) for _ in range(4)]
        sel = mm(seg_t[...], jnp.concatenate(hot, axis=0))
        for lt in range(half // LANES):
            g = geo[s, :, pl.ds(pl.multiple_of(h * half + lt * LANES, LANES), LANES)]
            g = [jnp.broadcast_to(g[i:i + 1], (8, LANES)) for i in range(9)]
            acc = [jnp.zeros((8, LANES), F32) for _ in range(6)]
            for r in range(LANES // 8):
                px, py, pz, nx, ny, nz = [
                    sel[q * LANES + r * 8:q * LANES + r * 8 + 8, lt * LANES:(lt + 1) * LANES]
                    for q in range(6)
                ]
                ox, oy, oz = g[0] - px, g[1] - py, g[2] - pz
                dist = ox * ox + oy * oy + oz * oz
                gap = ox * nx + oy * ny + oz * nz
                proj = jnp.abs(g[3] * nx + g[4] * ny + g[5] * nz)
                closing = g[6] * nx + g[7] * ny + g[8] * nz
                base = jnp.exp(-0.5 * dist) * jnp.maximum(-gap, 0.0) * proj
                damp = base * closing
                for k, n in enumerate((nx, ny, nz)):
                    acc[k] = acc[k] + base * n
                    acc[3 + k] = acc[3 + k] + damp * n
            sums = [jnp.sum(a, axis=0, keepdims=True) for a in acc]
            for k in range(6):
                sums_f[it * (half // LANES) + lt, k:k + 1, :] = sums[k]
        return carry

    lax.fori_loop(0, SIDES * halves, step, 0)

    for d in range(1, n_elem):
        cnt_copy(d - 1, lax.rem(me + n_elem - d, n_elem), me).wait_recv()
    whole = counts[0]
    for i in range(1, n_elem):
        whole = whole + counts[i]
    stiff = STIFFNESS * lax.rsqrt(jnp.maximum(whole[:, :buckets], 1.0))
    hi, mid, lo = split3(stiff)
    which = lax.broadcasted_iota(jnp.int32, stiff.shape, 0)
    stiff = jnp.where(which == 0, hi, jnp.where(which == 1, mid, jnp.where(which == 2, lo, 0.0)))
    stiff = mm(stiff.astype(BF16), onehot[...])
    stiff = (stiff[0:1] + stiff[1:2]) + stiff[2:3]
    for s in range(SIDES):
        for j in range(jblocks):
            at = s * count + j * LANES
            both = sums_f[s * jblocks + j]
            force = stiff[:, at:at + LANES] * both[0:3] - DAMPING * both[3:6]
            for k in range(3):
                parts[mb, k, j:j + 1, s * LANES:(s + 1) * LANES] = force[k:k + 1]

    def par_copy(slot, owner, target):
        return pltpu.make_async_remote_copy(
            src_ref=parts.at[owner], dst_ref=parts.at[owner],
            send_sem=par_send.at[slot], recv_sem=par_recv.at[slot],
            device_id={"bucket": target}, device_id_type=pl.DeviceIdType.MESH,
        )

    for d in range(1, n_buck):
        par_copy(d - 1, mb, lax.rem(mb + d, n_buck)).start()
    for d in range(1, n_buck):
        par_copy(d - 1, lax.rem(mb + n_buck - d, n_buck), mb).wait_recv()
    for k in range(3):
        force = parts[0, k]
        for i in range(1, n_buck):
            force = force + parts[i, k]
        for p, v in enumerate(split3(force)):
            at = (p * 3 + k) * jblocks
            inter[at:at + jblocks, :] = v
    used = 9 * jblocks
    if inter.shape[0] > used:
        inter[used:, :] = jnp.zeros((inter.shape[0] - used, BLOCK), F32)
    mixed = mm(inter[...].astype(BF16), perm[...], ((1,), (1,)))
    third = 3 * jblocks
    mixed = (mixed[0:third] + mixed[third:2 * third]) + mixed[2 * third:3 * third]
    for k in range(3):
        for j in range(jblocks):
            out[k:k + 1, j * BLOCK:(j + 1) * BLOCK] = mixed[k * jblocks + j:k * jblocks + j + 1]

    for d in range(1, n_elem):
        for cp in seg_copies(d - 1, d, me, lax.rem(me + d, n_elem)):
            cp.wait_send()
        cnt_copy(d - 1, me, lax.rem(me + d, n_elem)).wait_send()
    for d in range(1, n_buck):
        par_copy(d - 1, mb, lax.rem(mb + d, n_buck)).wait_send()


def local(n_elem, n_buck, node_data, eroded, bucket_map, seg_point, seg_angle):
    own, _, segs = seg_point.shape
    buckets = own * n_elem
    count = eroded.shape[0]
    jblocks = count // LANES
    elems = node_data.shape[1] // SIDES
    pad = -(-9 * jblocks // 16) * 16
    vmem = pl.BlockSpec(memory_space=pltpu.VMEM)
    dma = pltpu.SemaphoreType.DMA
    return pl.pallas_call(
        functools.partial(kernel, n_elem, n_buck),
        out_shape=jax.ShapeDtypeStruct((3, SIDES * count), F32),
        in_specs=[vmem] * 5,
        out_specs=vmem,
        scratch_shapes=[
            pltpu.VMEM((BLOCK, BLOCK), BF16),
            pltpu.VMEM((elems, count), BF16),
            pltpu.VMEM((3 * SIDES * ROWS, elems), BF16),
            pltpu.VMEM((SIDES, ROWS, count), F32),
            pltpu.VMEM((SIDES, 16, count), F32),
            pltpu.VMEM((buckets, SIDES * count), BF16),
            pltpu.VMEM((buckets, 3, segs), F32),
            pltpu.VMEM((buckets, 2, segs), F32),
            pltpu.VMEM((6 * segs, 4 * buckets), BF16),
            pltpu.VMEM((n_elem, 8, max(buckets, LANES)), F32),
            pltpu.VMEM((SIDES * jblocks, 8, LANES), F32),
            pltpu.VMEM((n_buck, 3, jblocks, BLOCK), F32),
            pltpu.VMEM((pad, BLOCK), F32),
            dma((2, n_elem - 1)),
            dma((2, n_elem - 1)),
            dma((n_elem - 1,)),
            dma((n_elem - 1,)),
            dma((n_buck - 1,)),
            dma((n_buck - 1,)),
        ],
        compiler_params=pltpu.CompilerParams(
            collective_id=0, has_side_effects=True, vmem_limit_bytes=60 * 1024 * 1024
        ),
        name="contact",
    )(node_data, eroded[None, :], bucket_map[None, :], seg_point, seg_angle)


def solution(mesh):
    in_specs = (
        P(None, "elem"),
        P("elem"),
        P("elem"),
        P("elem", None, "bucket"),
        P("elem", None, "bucket"),
    )
    body = functools.partial(local, mesh.shape["elem"], mesh.shape["bucket"])
    return jax.shard_map(
        body, mesh=mesh, in_specs=in_specs, out_specs=P(None, "elem"), check_vma=False
    )
```

```python
import functools

import jax
import jax.numpy as jnp
from jax import lax
from jax.experimental import pallas as pl
from jax.experimental.pallas import tpu as pltpu
from jax.sharding import PartitionSpec as P

STIFFNESS = 20.0
DAMPING = 0.5
LANES = 128
SIDES = 6
BLOCK = SIDES * LANES
F32 = jnp.float32
BF16 = jnp.bfloat16


def split3(x):
    hi = x.astype(BF16).astype(F32)
    rest = x - hi
    mid = rest.astype(BF16).astype(F32)
    return hi, mid, rest - mid


def sin_cos(x):
    k = jnp.floor(x * 0.6366197723675814 + 0.5)
    r = x - k * 1.5703125
    r = r - k * 4.837512969970703125e-4
    r = r - k * 7.54978995489188216e-8
    z = r * r
    s = ((-1.9515295891e-4 * z + 8.3321608736e-3) * z - 1.6666654611e-1) * z * r + r
    c = ((2.443315711809948e-5 * z - 1.388731625493765e-3) * z + 4.166664568298827e-2) * z * z
    c = c - 0.5 * z + 1.0
    q = k.astype(jnp.int32) & 3
    odd = (q & 1) == 1
    sin = jnp.where(odd, c, s)
    cos = jnp.where(odd, s, c)
    sin = jnp.where(q >= 2, -sin, sin)
    cos = jnp.where((q == 1) | (q == 2), -cos, cos)
    return sin, cos


def mm(a, b, contract=((1,), (0,))):
    return lax.dot_general(a, b, (contract, ((), ())), preferred_element_type=F32)


def kernel(
    n_elem, n_buck, node_any, eroded, bmap, spoint, sangle, out,
    node, perm, pick, rows, faces, onehot, points, angles, values, seg_t, counts,
    sel0, sel1, sums_f, parts, inter,
    node_sem, seg_send, seg_recv, cnt_send, cnt_recv, par_send, par_recv,
):
    me = lax.axis_index("elem")
    mb = lax.axis_index("bucket")
    own = sangle.shape[0]
    buckets = own * n_elem
    count = eroded.shape[1]
    jblocks = count // LANES
    blocks = node.shape[1] // BLOCK
    chunks = parts.shape[1]
    mesh_ids = pl.DeviceIdType.MESH

    barrier = pltpu.get_barrier_semaphore()
    for d in range(1, n_elem):
        to = {"elem": lax.rem(me + d, n_elem)}
        pl.semaphore_signal(barrier, inc=1, device_id=to, device_id_type=mesh_ids)
    for d in range(1, n_buck):
        to = {"bucket": lax.rem(mb + d, n_buck)}
        pl.semaphore_signal(barrier, inc=1, device_id=to, device_id_type=mesh_ids)
    fetch = pltpu.make_async_copy(node_any, node, node_sem)
    fetch.start()

    col = lax.broadcasted_iota(jnp.int32, (1, BLOCK), 1)
    source = SIDES * (col & (LANES - 1)) + (col // LANES)
    for i in range(BLOCK // 256):
        r = lax.broadcasted_iota(jnp.int32, (256, BLOCK), 0) + i * 256
        perm[i * 256:(i + 1) * 256, :] = jnp.where(r == source, 1.0, 0.0).astype(BF16)
    for i in range(pick.shape[0] // 256):
        r = lax.broadcasted_iota(jnp.int32, (256, count), 0) + i * 256
        pick[i * 256:(i + 1) * 256, :] = jnp.where(r == eroded[...], 1.0, 0.0).astype(BF16)

    pl.semaphore_wait(barrier, n_elem + n_buck - 2)

    def seg_copies(slot, owner, target):
        at = pl.ds(pl.multiple_of(owner * own, own), own)
        return [
            pltpu.make_async_remote_copy(
                src_ref=src, dst_ref=dst,
                send_sem=seg_send.at[i, slot], recv_sem=seg_recv.at[i, slot],
                device_id={"elem": target}, device_id_type=mesh_ids,
            )
            for i, (src, dst) in enumerate(
                [(spoint, points.at[:, at]), (sangle, angles.at[at])]
            )
        ]

    for d in range(1, n_elem):
        for c in seg_copies(d - 1, me, lax.rem(me + d, n_elem)):
            c.start()

    fetch.wait()
    group = 4
    for g in range(blocks // group):
        stack = []
        for i in range(g * group, (g + 1) * group):
            lanes = slice(i * BLOCK, (i + 1) * BLOCK)
            c = [node[3 * v:3 * v + 3, lanes] for v in range(8)]
            e1, e2 = c[2] - c[0], c[3] - c[1]
            r1 = jnp.concatenate([e1[1:3], e1[0:1]], axis=0)
            r2 = jnp.concatenate([e2[1:3], e2[0:1]], axis=0)
            area = 0.5 * (e1 * r2 - r1 * e2)
            centroid = 0.25 * (((c[0] + c[1]) + c[2]) + c[3])
            velocity = 0.25 * (((c[4] + c[5]) + c[6]) + c[7])
            ids = bmap[:, lanes].astype(F32)
            two = jnp.zeros((2, BLOCK), F32)
            four = jnp.zeros((4, BLOCK), F32)
            first = jnp.concatenate([centroid, area, two], axis=0)
            second = jnp.concatenate([velocity, ids, four], axis=0)
            a, b = split3(first), split3(second)
            stack += [a[0], b[0], a[1], b[1], a[2]]
        apart = mm(jnp.concatenate(stack, axis=0).astype(BF16), perm[...]).astype(BF16)
        for i in range(group):
            at = (g * group + i) * LANES
            for s in range(SIDES):
                rows[s * 40:(s + 1) * 40, at:at + LANES] = apart[
                    i * 40:(i + 1) * 40, s * LANES:(s + 1) * LANES
                ]

    taken = mm(rows[...], pick[...])
    for s in range(SIDES):
        t = [taken[s * 40 + i * 8:s * 40 + i * 8 + 8] for i in range(5)]
        faces[s, 0:8, :] = (t[0] + t[2]) + t[4]
        faces[s, 8:16, :] = t[1] + t[3]

    ones = jnp.ones((8, count), BF16)
    chunk = min(buckets, LANES)
    for b in range(0, buckets, chunk):
        iota = lax.broadcasted_iota(jnp.int32, (chunk, count), 0) + b
        total = jnp.zeros((chunk, count), F32)
        for s in range(SIDES):
            ids = faces[s, 11:12, :].astype(jnp.int32)
            hot = jnp.where(iota == ids, 1.0, 0.0)
            total = total + hot
            onehot[b:b + chunk, s * count:(s + 1) * count] = hot.astype(BF16)
        if chunk < LANES:
            total = jnp.concatenate([total, jnp.zeros((LANES - chunk, count), F32)], axis=0)
        counts[me, :, b:b + LANES] = mm(ones, total.astype(BF16), ((1,), (1,)))

    def cnt_copy(slot, owner, target):
        return pltpu.make_async_remote_copy(
            src_ref=counts.at[owner], dst_ref=counts.at[owner],
            send_sem=cnt_send.at[slot], recv_sem=cnt_recv.at[slot],
            device_id={"elem": target}, device_id_type=mesh_ids,
        )

    for d in range(1, n_elem):
        cnt_copy(d - 1, me, lax.rem(me + d, n_elem)).start()

    def unfold(owner, p, a):
        at = pl.ds(pl.multiple_of(owner * own, own), own)
        sin0, cos0 = sin_cos(a[:, 0, :])
        sin1, cos1 = sin_cos(a[:, 1, :])
        for i, v in enumerate([p[0], p[1], p[2], cos0 * sin1, sin0 * sin1, cos1]):
            values[i, at, :] = v

    unfold(me, spoint[...], sangle[...])
    order = sorted(range(1, n_elem), key=lambda d: min(d, n_elem - d))
    for d in order:
        owner = lax.rem(me + n_elem - d, n_elem)
        for cp in seg_copies(d - 1, owner, me):
            cp.wait_recv()
        at = pl.ds(pl.multiple_of(owner * own, own), own)
        unfold(owner, points[:, at, :], angles[at])

    chunk = min(buckets, LANES // 2)

    def lay_out(b):
        for i in range(6):
            v = values[i, pl.ds(pl.multiple_of(b * chunk, chunk), chunk), :]
            stack = jnp.concatenate(list(split3(v)) + [jnp.zeros_like(v)], axis=0)
            lanes = pl.ds(pl.multiple_of(b * 4 * chunk, LANES), 4 * chunk)
            seg_t[i * LANES:(i + 1) * LANES, lanes] = stack.T.astype(BF16)

    if buckets == chunk:
        lay_out(0)
    else:
        pl.loop(0, buckets // chunk)(lay_out)

    for d in range(1, n_elem):
        cnt_copy(d - 1, lax.rem(me + n_elem - d, n_elem), me).wait_recv()
    whole = counts[0]
    for i in range(1, n_elem):
        whole = whole + counts[i]
    stiff = STIFFNESS * lax.rsqrt(jnp.maximum(whole[:, :buckets], 1.0))
    hi, mid, lo = split3(stiff)
    which = lax.broadcasted_iota(jnp.int32, stiff.shape, 0)
    stiff = jnp.where(which == 0, hi, jnp.where(which == 1, mid, jnp.where(which == 2, lo, 0.0)))
    stiff = mm(stiff.astype(BF16), onehot[...])
    stiff = (stiff[0:1] + stiff[1:2]) + stiff[2:3]
    for s in range(SIDES):
        faces[s, 12:13, :] = stiff[:, s * count:(s + 1) * count]

    half = 256
    halves = count // half
    steps = SIDES * halves

    def select(it, sel):
        hot = onehot[:, pl.ds(pl.multiple_of(it * half, half), half)]
        hot = [hot[b:b + chunk] for b in range(0, buckets, chunk) for _ in range(4)]
        sel[...] = mm(seg_t[...], jnp.concatenate(hot, axis=0))

    def forces(it, sel):
        s = it // halves
        h = it % halves
        for lt in range(half // LANES):
            g = faces[s, :, pl.ds(pl.multiple_of(h * half + lt * LANES, LANES), LANES)]
            cx, cy, cz, az, ax, ay, _, _, vx, vy, vz, _, stf = [
                jnp.broadcast_to(g[i:i + 1], (8, LANES)) for i in range(13)
            ]
            vx, vy, vz = DAMPING * vx, DAMPING * vy, DAMPING * vz
            acc = [jnp.zeros((8, LANES), F32) for _ in range(3)]
            for r in range(LANES // 8):
                px, py, pz, nx, ny, nz = [
                    sel[q * LANES + r * 8:q * LANES + r * 8 + 8, lt * LANES:(lt + 1) * LANES]
                    for q in range(6)
                ]
                ox, oy, oz = px - cx, py - cy, pz - cz
                dist = ox * ox + oy * oy + oz * oz
                depth = jnp.maximum(ox * nx + oy * ny + oz * nz, 0.0)
                proj = jnp.abs(ax * nx + ay * ny + az * nz)
                push = stf - (vx * nx + vy * ny + vz * nz)
                traction = (jnp.exp(-0.5 * dist) * depth) * (push * proj)
                for k, n in enumerate((nx, ny, nz)):
                    acc[k] = acc[k] + traction * n
            for k in range(3):
                at = it * (half // LANES) + lt
                sums_f[at, k:k + 1, :] = jnp.sum(acc[k], axis=0, keepdims=True)

    def par_copy(c, slot, owner, target):
        return pltpu.make_async_remote_copy(
            src_ref=parts.at[owner, c], dst_ref=parts.at[owner, c],
            send_sem=par_send.at[c, slot], recv_sem=par_recv.at[c, slot],
            device_id={"bucket": target}, device_id_type=mesh_ids,
        )

    wide = SIDES // chunks
    select(0, sel0)
    for c in range(chunks):
        base = c * steps // chunks

        def step(i, carry):
            it = base + 2 * i
            select(it + 1, sel1)
            forces(it, sel0)
            select(lax.rem(it + 2, steps), sel0)
            forces(it + 1, sel1)
            return carry

        lax.fori_loop(0, steps // chunks // 2, step, 0)
        for s in range(wide):
            for j in range(jblocks):
                f = sums_f[(c * wide + s) * jblocks + j]
                for k in range(3):
                    parts[mb, c, k, j:j + 1, s * LANES:(s + 1) * LANES] = f[k:k + 1]
        for d in range(1, n_buck):
            par_copy(c, d - 1, mb, lax.rem(mb + d, n_buck)).start()

    for c in range(chunks):
        for d in range(1, n_buck):
            par_copy(c, d - 1, lax.rem(mb + n_buck - d, n_buck), mb).wait_recv()
        for k in range(3):
            force = parts[0, c, k]
            for i in range(1, n_buck):
                force = force + parts[i, c, k]
            for p, v in enumerate(split3(force)):
                at = (p * 3 + k) * jblocks
                inter[at:at + jblocks, c * wide * LANES:(c + 1) * wide * LANES] = v
    used = 9 * jblocks
    if inter.shape[0] > used:
        inter[used:, :] = jnp.zeros((inter.shape[0] - used, BLOCK), F32)
    mixed = mm(inter[...].astype(BF16), perm[...], ((1,), (1,)))
    third = 3 * jblocks
    mixed = (mixed[0:third] + mixed[third:2 * third]) + mixed[2 * third:3 * third]
    for k in range(3):
        for j in range(jblocks):
            out[k:k + 1, j * BLOCK:(j + 1) * BLOCK] = mixed[k * jblocks + j:k * jblocks + j + 1]

    for d in range(1, n_elem):
        for cp in seg_copies(d - 1, me, lax.rem(me + d, n_elem)):
            cp.wait_send()
        cnt_copy(d - 1, me, lax.rem(me + d, n_elem)).wait_send()
    for c in range(chunks):
        for d in range(1, n_buck):
            par_copy(c, d - 1, mb, lax.rem(mb + d, n_buck)).wait_send()


def local(n_elem, n_buck, node_data, eroded, bucket_map, seg_point, seg_angle):
    own, _, segs = seg_point.shape
    buckets = own * n_elem
    count = eroded.shape[0]
    jblocks = count // LANES
    elems = node_data.shape[1] // SIDES
    pad = -(-9 * jblocks // 16) * 16
    vmem = pl.BlockSpec(memory_space=pltpu.VMEM)
    dma = pltpu.SemaphoreType.DMA
    return pl.pallas_call(
        functools.partial(kernel, n_elem, n_buck),
        out_shape=jax.ShapeDtypeStruct((3, SIDES * count), F32),
        in_specs=[pl.BlockSpec(memory_space=pl.ANY)] + [vmem] * 4,
        out_specs=vmem,
        scratch_shapes=[
            pltpu.VMEM(node_data.shape, F32),
            pltpu.VMEM((BLOCK, BLOCK), BF16),
            pltpu.VMEM((elems, count), BF16),
            pltpu.VMEM((SIDES * 40, elems), BF16),
            pltpu.VMEM((SIDES, 16, count), F32),
            pltpu.VMEM((buckets, SIDES * count), BF16),
            pltpu.VMEM((3, buckets, segs), F32),
            pltpu.VMEM((buckets, 2, segs), F32),
            pltpu.VMEM((6, buckets, segs), F32),
            pltpu.VMEM((6 * segs, 4 * buckets), BF16),
            pltpu.VMEM((n_elem, 8, max(buckets, LANES)), F32),
            pltpu.VMEM((6 * segs, 256), F32),
            pltpu.VMEM((6 * segs, 256), F32),
            pltpu.VMEM((SIDES * jblocks, 8, LANES), F32),
            pltpu.VMEM((n_buck, 3, 3, jblocks, BLOCK // 3), F32),
            pltpu.VMEM((pad, BLOCK), F32),
            dma,
            dma((2, n_elem - 1)),
            dma((2, n_elem - 1)),
            dma((n_elem - 1,)),
            dma((n_elem - 1,)),
            dma((3, n_buck - 1)),
            dma((3, n_buck - 1)),
        ],
        compiler_params=pltpu.CompilerParams(
            collective_id=0, has_side_effects=True, vmem_limit_bytes=60 * 1024 * 1024
        ),
        name="contact",
    )(node_data, eroded[None, :], bucket_map[None, :], seg_point.transpose(1, 0, 2), seg_angle)


def solution(mesh):
    in_specs = (
        P(None, "elem"),
        P("elem"),
        P("elem"),
        P("elem", None, "bucket"),
        P("elem", None, "bucket"),
    )
    body = functools.partial(local, mesh.shape["elem"], mesh.shape["bucket"])
    return jax.shard_map(
        body, mesh=mesh, in_specs=in_specs, out_specs=P(None, "elem"), check_vma=False
    )
```

```python
import functools

import jax
import jax.numpy as jnp
from jax import lax
from jax.experimental import pallas as pl
from jax.experimental.pallas import tpu as pltpu
from jax.sharding import PartitionSpec as P

STIFFNESS = 20.0
DAMPING = 0.5
HALF_LOG2E = -0.7213475204444817
LANES = 128
SIDES = 6
BLOCK = SIDES * LANES
F32 = jnp.float32
BF16 = jnp.bfloat16


def split3(x):
    hi = x.astype(BF16).astype(F32)
    rest = x - hi
    mid = rest.astype(BF16).astype(F32)
    return hi, mid, rest - mid


def sin_cos(x):
    k = jnp.floor(x * 0.6366197723675814 + 0.5)
    r = x - k * 1.5703125
    r = r - k * 4.837512969970703125e-4
    r = r - k * 7.54978995489188216e-8
    z = r * r
    s = ((-1.9515295891e-4 * z + 8.3321608736e-3) * z - 1.6666654611e-1) * z * r + r
    c = ((2.443315711809948e-5 * z - 1.388731625493765e-3) * z + 4.166664568298827e-2) * z * z
    c = c - 0.5 * z + 1.0
    q = k.astype(jnp.int32) & 3
    odd = (q & 1) == 1
    sin = jnp.where(odd, c, s)
    cos = jnp.where(odd, s, c)
    sin = jnp.where(q >= 2, -sin, sin)
    cos = jnp.where((q == 1) | (q == 2), -cos, cos)
    return sin, cos


def mm(a, b, contract=((1,), (0,))):
    return lax.dot_general(a, b, (contract, ((), ())), preferred_element_type=F32)


def kernel(
    n_elem, n_buck, node_any, eroded, bmap, spoint, sangle, out,
    node, perm, pick, rows, faces, onehot, points, angles, values, seg_t, counts,
    sel0, sel1, sums_f, parts, inter,
    node_sem, seg_send, seg_recv, cnt_send, cnt_recv, par_send, par_recv,
):
    me = lax.axis_index("elem")
    mb = lax.axis_index("bucket")
    own = sangle.shape[0]
    buckets = own * n_elem
    count = eroded.shape[1]
    jblocks = count // LANES
    blocks = node.shape[1] // BLOCK
    chunks = parts.shape[1]
    mesh_ids = pl.DeviceIdType.MESH

    barrier = pltpu.get_barrier_semaphore()
    for d in range(1, n_elem):
        to = {"elem": lax.rem(me + d, n_elem)}
        pl.semaphore_signal(barrier, inc=1, device_id=to, device_id_type=mesh_ids)
    for d in range(1, n_buck):
        to = {"bucket": lax.rem(mb + d, n_buck)}
        pl.semaphore_signal(barrier, inc=1, device_id=to, device_id_type=mesh_ids)
    fetch = pltpu.make_async_copy(node_any, node, node_sem)
    fetch.start()

    col = lax.broadcasted_iota(jnp.int32, (1, BLOCK), 1)
    source = SIDES * (col & (LANES - 1)) + (col // LANES)
    for i in range(BLOCK // 256):
        r = lax.broadcasted_iota(jnp.int32, (256, BLOCK), 0) + i * 256
        perm[i * 256:(i + 1) * 256, :] = jnp.where(r == source, 1.0, 0.0).astype(BF16)
    for i in range(pick.shape[0] // 256):
        r = lax.broadcasted_iota(jnp.int32, (256, count), 0) + i * 256
        pick[i * 256:(i + 1) * 256, :] = jnp.where(r == eroded[...], 1.0, 0.0).astype(BF16)

    def seg_copies(slot, owner, target):
        at = pl.ds(pl.multiple_of(owner * own, own), own)
        return [
            pltpu.make_async_remote_copy(
                src_ref=src, dst_ref=dst,
                send_sem=seg_send.at[i, slot], recv_sem=seg_recv.at[i, slot],
                device_id={"elem": target}, device_id_type=mesh_ids,
            )
            for i, (src, dst) in enumerate(
                [(spoint, points.at[:, at]), (sangle, angles.at[at])]
            )
        ]

    fetch.wait()
    group = 4
    order = sorted(range(1, n_elem), key=lambda d: min(d, n_elem - d))
    for g in range(blocks // group):
        if g == blocks // group // 2:
            pl.semaphore_wait(barrier, n_elem + n_buck - 2)
            for d in reversed(order):
                for cp in seg_copies(d - 1, me, lax.rem(me + d, n_elem)):
                    cp.start()
        stack = []
        for i in range(g * group, (g + 1) * group):
            lanes = slice(i * BLOCK, (i + 1) * BLOCK)
            c = [node[3 * v:3 * v + 3, lanes] for v in range(8)]
            e1, e2 = c[2] - c[0], c[3] - c[1]
            r1 = jnp.concatenate([e1[1:3], e1[0:1]], axis=0)
            r2 = jnp.concatenate([e2[1:3], e2[0:1]], axis=0)
            area = 0.5 * (e1 * r2 - r1 * e2)
            centroid = 0.25 * (((c[0] + c[1]) + c[2]) + c[3])
            velocity = 0.25 * (((c[4] + c[5]) + c[6]) + c[7])
            ids = bmap[:, lanes].astype(F32)
            two = jnp.zeros((2, BLOCK), F32)
            four = jnp.zeros((4, BLOCK), F32)
            first = jnp.concatenate([centroid, area, two], axis=0)
            second = jnp.concatenate([velocity, ids, four], axis=0)
            a, b = split3(first), split3(second)
            stack += [a[0], b[0], a[1], b[1], a[2]]
        apart = mm(jnp.concatenate(stack, axis=0).astype(BF16), perm[...]).astype(BF16)
        for i in range(group):
            at = (g * group + i) * LANES
            for s in range(SIDES):
                rows[s * 40:(s + 1) * 40, at:at + LANES] = apart[
                    i * 40:(i + 1) * 40, s * LANES:(s + 1) * LANES
                ]

    taken = mm(rows[...], pick[...])
    for s in range(SIDES):
        t = [taken[s * 40 + i * 8:s * 40 + i * 8 + 8] for i in range(5)]
        faces[s, 0:8, :] = (t[0] + t[2]) + t[4]
        faces[s, 8:16, :] = t[1] + t[3]

    ones = jnp.ones((8, count), BF16)
    chunk = min(buckets, LANES)
    for b in range(0, buckets, chunk):
        iota = lax.broadcasted_iota(jnp.int32, (chunk, count), 0) + b
        total = jnp.zeros((chunk, count), F32)
        for s in range(SIDES):
            ids = faces[s, 11:12, :].astype(jnp.int32)
            hot = jnp.where(iota == ids, 1.0, 0.0)
            total = total + hot
            onehot[b:b + chunk, s * count:(s + 1) * count] = hot.astype(BF16)
        if chunk < LANES:
            total = jnp.concatenate([total, jnp.zeros((LANES - chunk, count), F32)], axis=0)
        counts[me, :, b:b + LANES] = mm(ones, total.astype(BF16), ((1,), (1,)))[0:1]

    def cnt_copy(slot, owner, target):
        return pltpu.make_async_remote_copy(
            src_ref=counts.at[owner], dst_ref=counts.at[owner],
            send_sem=cnt_send.at[slot], recv_sem=cnt_recv.at[slot],
            device_id={"elem": target}, device_id_type=mesh_ids,
        )

    for d in range(1, n_elem):
        cnt_copy(d - 1, me, lax.rem(me + d, n_elem)).start()

    def unfold(owner, p, a):
        at = pl.ds(pl.multiple_of(owner * own, own), own)
        sin0, cos0 = sin_cos(a[:, 0, :])
        sin1, cos1 = sin_cos(a[:, 1, :])
        for i, v in enumerate([p[0], p[1], p[2], cos0 * sin1, sin0 * sin1, cos1]):
            values[i, at, :] = v

    unfold(me, spoint[...], sangle[...])
    for d in order:
        owner = lax.rem(me + n_elem - d, n_elem)
        for cp in seg_copies(d - 1, owner, me):
            cp.wait_recv()
        at = pl.ds(pl.multiple_of(owner * own, own), own)
        unfold(owner, points[:, at, :], angles[at])

    chunk = min(buckets, LANES // 2)

    def lay_out(b):
        for i in range(6):
            v = values[i, pl.ds(pl.multiple_of(b * chunk, chunk), chunk), :]
            stack = jnp.concatenate(list(split3(v)) + [jnp.zeros_like(v)], axis=0)
            lanes = pl.ds(pl.multiple_of(b * 4 * chunk, LANES), 4 * chunk)
            seg_t[i * LANES:(i + 1) * LANES, lanes] = stack.T.astype(BF16)

    if buckets == chunk:
        lay_out(0)
    else:
        pl.loop(0, buckets // chunk)(lay_out)

    for d in range(1, n_elem):
        cnt_copy(d - 1, lax.rem(me + n_elem - d, n_elem), me).wait_recv()
    whole = counts[0]
    for i in range(1, n_elem):
        whole = whole + counts[i]
    whole = jnp.broadcast_to(whole[:, :buckets], (8, buckets))
    stiff = STIFFNESS * lax.rsqrt(jnp.maximum(whole, 1.0))
    hi, mid, lo = split3(stiff)
    which = lax.broadcasted_iota(jnp.int32, stiff.shape, 0)
    stiff = jnp.where(which == 0, hi, jnp.where(which == 1, mid, jnp.where(which == 2, lo, 0.0)))
    stiff = mm(stiff.astype(BF16), onehot[...])
    stiff = (stiff[0:1] + stiff[1:2]) + stiff[2:3]
    for s in range(SIDES):
        faces[s, 12:13, :] = stiff[:, s * count:(s + 1) * count]

    half = 256
    halves = count // half
    steps = SIDES * halves

    def select(it, sel):
        hot = onehot[:, pl.ds(pl.multiple_of(it * half, half), half)]
        hot = [hot[b:b + chunk] for b in range(0, buckets, chunk) for _ in range(4)]
        sel[...] = mm(seg_t[...], jnp.concatenate(hot, axis=0))

    def forces(it, sel):
        s = it // halves
        h = it % halves
        for lt in range(half // LANES):
            g = faces[s, :, pl.ds(pl.multiple_of(h * half + lt * LANES, LANES), LANES)]
            cx, cy, cz, az, ax, ay, _, _, vx, vy, vz, _, stf = [
                jnp.broadcast_to(g[i:i + 1], (8, LANES)) for i in range(13)
            ]
            vx, vy, vz = DAMPING * vx, DAMPING * vy, DAMPING * vz
            acc = [jnp.zeros((8, LANES), F32) for _ in range(3)]
            for r in range(LANES // 8):
                px, py, pz, nx, ny, nz = [
                    sel[q * LANES + r * 8:q * LANES + r * 8 + 8, lt * LANES:(lt + 1) * LANES]
                    for q in range(6)
                ]
                ox, oy, oz = px - cx, py - cy, pz - cz
                dist = ox * ox + oy * oy + oz * oz
                depth = jnp.maximum(ox * nx + oy * ny + oz * nz, 0.0)
                proj = jnp.abs(ax * nx + ay * ny + az * nz)
                push = stf - (vx * nx + vy * ny + vz * nz)
                traction = (jnp.exp2(HALF_LOG2E * dist) * depth) * (push * proj)
                for k, n in enumerate((nx, ny, nz)):
                    acc[k] = acc[k] + traction * n
            for k in range(3):
                at = it * (half // LANES) + lt
                sums_f[at, k:k + 1, :] = jnp.sum(acc[k], axis=0, keepdims=True)

    def par_copy(c, slot, owner, target):
        return pltpu.make_async_remote_copy(
            src_ref=parts.at[owner, c], dst_ref=parts.at[owner, c],
            send_sem=par_send.at[c, slot], recv_sem=par_recv.at[c, slot],
            device_id={"bucket": target}, device_id_type=mesh_ids,
        )

    wide = SIDES // chunks
    select(0, sel0)
    for c in range(chunks):
        base = c * steps // chunks

        def step(i, carry):
            it = base + 2 * i
            select(it + 1, sel1)
            forces(it, sel0)
            select(lax.rem(it + 2, steps), sel0)
            forces(it + 1, sel1)
            return carry

        lax.fori_loop(0, steps // chunks // 2, step, 0)
        for s in range(wide):
            for j in range(jblocks):
                f = sums_f[(c * wide + s) * jblocks + j]
                for k in range(3):
                    parts[mb, c, k, j:j + 1, s * LANES:(s + 1) * LANES] = f[k:k + 1]
        for d in range(1, n_buck):
            par_copy(c, d - 1, mb, lax.rem(mb + d, n_buck)).start()

    for c in range(chunks):
        for d in range(1, n_buck):
            par_copy(c, d - 1, lax.rem(mb + n_buck - d, n_buck), mb).wait_recv()
        for k in range(3):
            force = parts[0, c, k]
            for i in range(1, n_buck):
                force = force + parts[i, c, k]
            for p, v in enumerate(split3(force)):
                at = (p * 3 + k) * jblocks
                inter[at:at + jblocks, c * wide * LANES:(c + 1) * wide * LANES] = v
    used = 9 * jblocks
    if inter.shape[0] > used:
        inter[used:, :] = jnp.zeros((inter.shape[0] - used, BLOCK), F32)
    mixed = mm(inter[...].astype(BF16), perm[...], ((1,), (1,)))
    third = 3 * jblocks
    mixed = (mixed[0:third] + mixed[third:2 * third]) + mixed[2 * third:3 * third]
    for k in range(3):
        for j in range(jblocks):
            out[k:k + 1, j * BLOCK:(j + 1) * BLOCK] = mixed[k * jblocks + j:k * jblocks + j + 1]

    for d in range(1, n_elem):
        for cp in seg_copies(d - 1, me, lax.rem(me + d, n_elem)):
            cp.wait_send()
        cnt_copy(d - 1, me, lax.rem(me + d, n_elem)).wait_send()
    for c in range(chunks):
        for d in range(1, n_buck):
            par_copy(c, d - 1, mb, lax.rem(mb + d, n_buck)).wait_send()


def local(n_elem, n_buck, node_data, eroded, bucket_map, seg_point, seg_angle):
    own, _, segs = seg_point.shape
    buckets = own * n_elem
    count = eroded.shape[0]
    jblocks = count // LANES
    elems = node_data.shape[1] // SIDES
    pad = -(-9 * jblocks // 16) * 16
    vmem = pl.BlockSpec(memory_space=pltpu.VMEM)
    dma = pltpu.SemaphoreType.DMA
    return pl.pallas_call(
        functools.partial(kernel, n_elem, n_buck),
        out_shape=jax.ShapeDtypeStruct((3, SIDES * count), F32),
        in_specs=[pl.BlockSpec(memory_space=pl.ANY)] + [vmem] * 4,
        out_specs=vmem,
        scratch_shapes=[
            pltpu.VMEM(node_data.shape, F32),
            pltpu.VMEM((BLOCK, BLOCK), BF16),
            pltpu.VMEM((elems, count), BF16),
            pltpu.VMEM((SIDES * 40, elems), BF16),
            pltpu.VMEM((SIDES, 16, count), F32),
            pltpu.VMEM((buckets, SIDES * count), BF16),
            pltpu.VMEM((3, buckets, segs), F32),
            pltpu.VMEM((buckets, 2, segs), F32),
            pltpu.VMEM((6, buckets, segs), F32),
            pltpu.VMEM((6 * segs, 4 * buckets), BF16),
            pltpu.VMEM((n_elem, 1, max(buckets, LANES)), F32),
            pltpu.VMEM((6 * segs, 256), F32),
            pltpu.VMEM((6 * segs, 256), F32),
            pltpu.VMEM((SIDES * jblocks, 8, LANES), F32),
            pltpu.VMEM((n_buck, 3, 3, jblocks, BLOCK // 3), F32),
            pltpu.VMEM((pad, BLOCK), F32),
            dma,
            dma((2, n_elem - 1)),
            dma((2, n_elem - 1)),
            dma((n_elem - 1,)),
            dma((n_elem - 1,)),
            dma((3, n_buck - 1)),
            dma((3, n_buck - 1)),
        ],
        compiler_params=pltpu.CompilerParams(
            collective_id=0, has_side_effects=True, vmem_limit_bytes=60 * 1024 * 1024
        ),
        name="contact",
    )(node_data, eroded[None, :], bucket_map[None, :], seg_point.transpose(1, 0, 2), seg_angle)


def solution(mesh):
    in_specs = (
        P(None, "elem"),
        P("elem"),
        P("elem"),
        P("elem", None, "bucket"),
        P("elem", None, "bucket"),
    )
    body = functools.partial(local, mesh.shape["elem"], mesh.shape["bucket"])
    return jax.shard_map(
        body, mesh=mesh, in_specs=in_specs, out_specs=P(None, "elem"), check_vma=False
    )
```
